32 devices in a mesh: row: 4 (over x, core), col: 8 (over z, y).
Axes of the slice: x: 2, y: 2, z: 4, core: 2. Of those that a mesh axis runs over, the one named last changes fastest.
Arguments:
- users: bfloat16 [32768, 256], P(('row', 'col')), may hold values from -20 to 20
- positives: int32 [32768], P(('row', 'col')), may hold values from 0 to 511
- items: bfloat16 [512, 256], P(('row', 'col')), may hold values from -6 to 6
- item_ids: int32 [512], P(('row', 'col')), may hold values from 0 to 999999
Outputs:
- loss: float32 [32768], P(('row', 'col'))
The draws below stay inside these ranges and needn't reach their ends.
All inputs are finite; a program needn't handle non-finite values.
Results may differ from the reference program's by a relative error of at most 0.0003.
Values may be sent and summed in bfloat16 or wider, within the bound.
No kernel may reach another device: no remote copies, remote signals or barrier semaphores. Data moves between devices by JAX's collectives and lax.ppermute only.
A program may use at most 128 MiB of HBM per device.

```python
import math
import jax
import jax.numpy as jnp
import numpy as np
from jax import lax

E = 256
ITEMS_DEV = 16
USERS = 32768
ITEMS = 512


def drawn(key):
    item_key = jax.random.fold_in(key, 11)
    user_key = jax.random.fold_in(key, 12)
    items = jnp.clip(jax.random.normal(item_key, (ITEMS, E), jnp.float32), -6.0, 6.0)
    users = jnp.clip(jax.random.normal(user_key, (USERS, E), jnp.float32), -6.0, 6.0)
    return (users, items)


def draw_users(key, part):
    return drawn(key)[0].astype(jnp.bfloat16)


def draw_items(key, part):
    return drawn(key)[1].astype(jnp.bfloat16)


def place_ends(drawn, own_key, low, high):
    spot = [jax.random.randint(jax.random.fold_in(own_key, axis), (), 0, length) for axis, length in enumerate(drawn.shape)]
    widest = drawn.shape.index(max(drawn.shape))
    neighbour = spot[:widest] + [(spot[widest] + 1) % drawn.shape[widest]] + spot[widest + 1:]
    return drawn.at[tuple(spot)].set(low).at[tuple(neighbour)].set(high)


def wide_ids(rng, shape, count, lean):
    portions = [min(1 << octave, count + 1 - (1 << octave)) * (1 << 20) // math.isqrt((1 << octave) ** lean) + 1 for octave in range((count + 1).bit_length()) if 1 << octave <= count]
    scale = 1 + sum(portions) // (1 << 30)
    listing = np.cumsum(np.array([max(1, weight // scale) for weight in portions]))
    ticket = jax.random.randint(jax.random.fold_in(rng, 1), shape, 0, int(listing[len(portions) - 1]))
    start = jnp.left_shift(1, jnp.searchsorted(jnp.asarray(listing, jnp.int32), ticket, side="right").astype(jnp.int32))
    rank = start - 1 + jax.random.randint(jax.random.fold_in(rng, 4), shape, 0, 1 << 30) % jnp.minimum(start, count + 1 - start)
    return jax.random.permutation(jax.random.fold_in(rng, 2), count)[rank].astype(jnp.int32)


def setup_inputs(seed: int = 0) -> dict:
    key_list = jax.random.split(jax.random.key(seed), 5)
    users = draw_users(jax.random.fold_in(key_list[4], 71), 0)
    positives = place_ends(jax.random.randint(key_list[1], (USERS,), 0, ITEMS), jax.random.fold_in(key_list[1], 1), 0, ITEMS - 1).astype(jnp.int32)
    items = draw_items(jax.random.fold_in(key_list[4], 71), 0)
    item_ids = place_ends(wide_ids(key_list[3], (ITEMS,), 1000000, 2), jax.random.fold_in(key_list[3], 3), 0, 999999).astype(jnp.int32)
    return {"users": users, "positives": positives, "items": items, "item_ids": item_ids}


def reference(users, positives, items, item_ids):
    pos_id = item_ids[positives]
    block = ITEMS_DEV * 8
    count = ITEMS // block
    init = (jnp.full((USERS,), -1e30, jnp.float32), jnp.zeros((USERS,), jnp.float32), jnp.zeros((USERS,), jnp.float32))

    def step(carry, index):
        high, summed, chosen = carry
        start = (index * block).astype(jnp.int32)
        piece = lax.dynamic_slice_in_dim(items, start, block, 0)
        ids = lax.dynamic_slice_in_dim(item_ids, start, block, 0)
        where_at = start + jnp.arange(block, dtype=jnp.int32)
        scores = 0.125 * jnp.dot(users, piece.T, preferred_element_type=jnp.float32)
        hit = where_at[None, :] == positives[:, None]
        keep = (ids[None, :] != pos_id[:, None]) | hit
        masked = jnp.where(keep, scores, -1e30)
        new_high = jnp.maximum(high, jnp.max(masked, axis=1))
        terms = jnp.where(keep, jnp.exp(masked - new_high[:, None]), 0.0)
        summed = summed * jnp.exp(high - new_high) + jnp.sum(terms, axis=1)
        chosen = chosen + jnp.sum(jnp.where(hit, scores, 0.0), axis=1)
        return (new_high, summed, chosen), None

    carry, _ = lax.scan(step, init, jnp.arange(count, dtype=jnp.int32))
    high, summed, chosen = carry
    return high + jnp.log(summed) - chosen
```

```python
import functools
import math

import jax
import jax.numpy as jnp
from jax import lax
from jax.experimental import pallas as pl
from jax.experimental.pallas import tpu as pltpu
from jax.sharding import PartitionSpec as P

LANES = 128
SUB = 8
BASE = 256
DIGITS = 3
LOW = -1e30


def pack_kernel(items_ref, ids_ref, out_ref):
    rows, width = items_ref.shape
    groups = rows // SUB
    span = LANES // groups
    copies = out_ref.shape[0]
    row = lax.broadcasted_iota(jnp.int32, (SUB, LANES), 0)
    lane = lax.broadcasted_iota(jnp.int32, (SUB, LANES), 1)
    held = jnp.zeros((SUB, LANES), jnp.int32)
    for k in range(rows):
        group = k // SUB
        mine = (row == k % SUB) & (lane >= group * span) & (lane < (group + 1) * span)
        held = jnp.where(mine, ids_ref[k], held)
    place = lane % span
    digit = jnp.zeros((SUB, LANES), jnp.int32)
    for d in range(DIGITS):
        digit = jnp.where(place == d, (held // BASE**d) % BASE, digit)
    tail = digit.astype(jnp.float32).astype(jnp.bfloat16)
    cols = [items_ref[:, c * LANES : (c + 1) * LANES] for c in range(width // LANES)]
    for n in range(copies):
        for c, col in enumerate(cols):
            out_ref[n, c * rows : (c + 1) * rows, :] = col
        out_ref[n, len(cols) * rows :, :] = tail


def pack(items, ids, copies):
    rows, width = items.shape
    tall = rows * (width // LANES) + SUB
    return pl.pallas_call(
        pack_kernel,
        out_shape=jax.ShapeDtypeStruct((copies, tall, LANES), items.dtype),
        in_specs=[
            pl.BlockSpec(memory_space=pltpu.VMEM),
            pl.BlockSpec(memory_space=pltpu.SMEM),
        ],
        out_specs=pl.BlockSpec(memory_space=pltpu.VMEM),
        compiler_params=pltpu.CompilerParams(vmem_limit_bytes=(2 << 20) + 4 * copies * tall * LANES),
        name="pack",
    )(items, ids)


def repeat(count, body, init):
    return body(0, init) if count == 1 else lax.fori_loop(0, count, body, init)


def loss_kernel(rows, pool_ref, users_ref, pos_ref, out_ref, score_ref, id_ref):
    devices = pool_ref.shape[0]
    users, width = users_ref.shape
    cols = width // LANES
    groups = rows // SUB
    span = LANES // groups
    wide = score_ref.shape[1]
    batch = math.gcd(devices, max(1, 512 // rows))
    blocks = devices // batch
    tiles = batch * groups
    rate = 0.125 / math.log(2)

    k = lax.broadcasted_iota(jnp.int32, (LANES, groups * LANES), 0)
    g = lax.broadcasted_iota(jnp.int32, (LANES, groups * LANES), 1) // LANES
    weigh = jnp.zeros((LANES, groups * LANES), jnp.float32)
    for d in range(DIGITS):
        weigh = jnp.where(k == g * span + d, float(BASE**d), weigh)
    weigh = weigh.astype(jnp.bfloat16)

    def decode(b, _):
        digit = pool_ref[pl.ds(b * batch, batch), cols * rows :, :].reshape(batch * SUB, LANES)
        id_ref[pl.ds(b * batch * SUB, batch * SUB), :] = jnp.dot(
            digit, weigh, preferred_element_type=jnp.float32
        )
        return 0

    repeat(blocks, decode, 0)

    def ids(b, t):
        d, g = divmod(t, groups)
        return id_ref[pl.ds((b * batch + d) * SUB, SUB), g * LANES : (g + 1) * LANES]

    up = lax.broadcasted_iota(jnp.int32, (SUB, LANES), 0)
    zero = jnp.zeros((SUB, LANES), jnp.float32)

    for u in range(users // wide):

        def multiply(b, _):
            pool = jnp.concatenate(
                [
                    pool_ref[pl.ds(b * batch, batch), c * rows : (c + 1) * rows, :].reshape(batch * rows, LANES)
                    for c in range(cols)
                ],
                axis=1,
            )
            score_ref[pl.ds(b * batch * rows, batch * rows), :] = lax.dot_general(
                pool, users_ref[u * wide : (u + 1) * wide, :], (((1,), (1,)), ((), ())),
                preferred_element_type=jnp.float32,
            )
            return 0

        repeat(blocks, multiply, 0)
        for v in range(wide // LANES):
            at = u * wide + v * LANES

            def place(b, t):
                return pl.ds((b * tiles + t) * SUB, SUB), slice(v * LANES, (v + 1) * LANES)

            def find(b, carry):
                own, got = carry
                where = pos_ref[:, at : at + LANES] - (up + b * tiles * SUB)
                for t in range(tiles):
                    hit = where == t * SUB
                    own = own + jnp.where(hit, ids(b, t), 0.0)
                    got = got + jnp.where(hit, score_ref[place(b, t)], 0.0)
                return own, got

            own, got = repeat(blocks, find, (zero, zero))
            own = jnp.broadcast_to(jnp.sum(own, axis=0, keepdims=True), (SUB, LANES))
            got = jnp.sum(got, axis=0, keepdims=True)

            def mask(b, high):
                for t in range(tiles):
                    masked = jnp.where(ids(b, t) == own, LOW, score_ref[place(b, t)])
                    score_ref[place(b, t)] = masked
                    high = jnp.maximum(high, masked)
                return high

            high = repeat(blocks, mask, zero + LOW)
            top = jnp.maximum(jnp.max(high, axis=0, keepdims=True), got)
            high = jnp.broadcast_to(top, (SUB, LANES))

            def add(b, summed):
                for t in range(tiles):
                    summed = summed + jnp.exp2((score_ref[place(b, t)] - high) * rate)
                return summed

            summed = jnp.sum(repeat(blocks, add, zero), axis=0, keepdims=True)
            summed = summed + jnp.exp2((got - top) * rate)
            out_ref[:, at : at + LANES] = 0.125 * (top - got) + jnp.log(summed)


def losses(pool, users, positives, rows):
    devices = pool.shape[0]
    count, _ = users.shape
    wide = min(count, 2 * LANES)
    limit = (8 << 20) + 4 * devices * rows * wide + 4 * devices * rows * LANES + 2 * pool.nbytes
    return pl.pallas_call(
        functools.partial(loss_kernel, rows),
        out_shape=jax.ShapeDtypeStruct((1, count), jnp.float32),
        in_specs=[pl.BlockSpec(memory_space=pltpu.VMEM)] * 3,
        out_specs=pl.BlockSpec(memory_space=pltpu.VMEM),
        scratch_shapes=[
            pltpu.VMEM((devices * rows, wide), jnp.float32),
            pltpu.VMEM((devices * SUB, rows // SUB * LANES), jnp.float32),
        ],
        compiler_params=pltpu.CompilerParams(vmem_limit_bytes=limit),
        name="losses",
    )(pool, users, positives.reshape(1, count)).reshape(count)


def per_device(axes, devices, users, positives, items, item_ids):
    rows = items.shape[0]
    sent = pack(items, item_ids, devices)
    pool = lax.all_to_all(sent, axes, 0, 0, tiled=False)
    return losses(pool, users, positives, rows)


def solution(mesh):
    axes = ("row", "col")
    devices = mesh.shape["row"] * mesh.shape["col"]
    both = P(axes)
    return jax.shard_map(
        functools.partial(per_device, axes, devices),
        mesh=mesh,
        in_specs=(P(axes, None), both, P(axes, None), both),
        out_specs=both,
        check_vma=False,
    )
```

```python
import functools
import math
import random

import jax
import jax.numpy as jnp
from jax import lax
from jax.experimental import pallas as pl
from jax.experimental.pallas import tpu as pltpu
from jax.sharding import Mesh
from jax.sharding import PartitionSpec as P

LANES = 128
SUB = 8
BASE = 256
DIGITS = 3
LOW = -1e30
RATE = 0.125 / math.log(2)
SEED = 126


def pack_kernel(items_hbm, ids_hbm, out_ref, items_ref, ids_ref, sems):
    rows, width = items_ref.shape
    groups = rows // SUB
    span = LANES // groups
    copies = out_ref.shape[0]
    get_items = pltpu.make_async_copy(items_hbm, items_ref, sems.at[0])
    get_ids = pltpu.make_async_copy(ids_hbm, ids_ref, sems.at[1])
    get_ids.start()
    get_items.start()
    row = lax.broadcasted_iota(jnp.int32, (SUB, LANES), 0)
    lane = lax.broadcasted_iota(jnp.int32, (SUB, LANES), 1)
    get_ids.wait()
    held = jnp.zeros((SUB, LANES), jnp.int32)
    for k in range(rows):
        group = k // SUB
        mine = (row == k % SUB) & (lane >= group * span) & (lane < (group + 1) * span)
        held = jnp.where(mine, ids_ref[k], held)
    place = lane % span
    digit = jnp.zeros((SUB, LANES), jnp.int32)
    for d in range(DIGITS):
        digit = jnp.where(place == d, (held // BASE**d) % BASE, digit)
    tail = digit.astype(jnp.float32).astype(jnp.bfloat16)
    get_items.wait()
    cols = [items_ref[:, c * LANES : (c + 1) * LANES] for c in range(width // LANES)]
    for n in range(copies):
        for c, col in enumerate(cols):
            out_ref[n, c * rows : (c + 1) * rows, :] = col
        out_ref[n, len(cols) * rows :, :] = tail


def pack(items, ids, copies):
    rows, width = items.shape
    tall = rows * (width // LANES) + SUB
    return pl.pallas_call(
        pack_kernel,
        out_shape=jax.ShapeDtypeStruct((copies, tall, LANES), items.dtype),
        in_specs=[pl.BlockSpec(memory_space=pltpu.HBM)] * 2,
        out_specs=pl.BlockSpec(memory_space=pltpu.VMEM),
        scratch_shapes=[
            pltpu.VMEM((rows, width), items.dtype),
            pltpu.SMEM((rows,), jnp.int32),
            pltpu.SemaphoreType.DMA((2,)),
        ],
        compiler_params=pltpu.CompilerParams(vmem_limit_bytes=(2 << 20) + 4 * copies * tall * LANES),
        cost_estimate=pl.CostEstimate(flops=1 << 30, bytes_accessed=1 << 22, transcendentals=0),
        name="pack",
    )(pltpu.with_memory_space_constraint(items, pltpu.HBM), pltpu.with_memory_space_constraint(ids, pltpu.HBM))


def chunk_of(chips, rows):
    return math.gcd(chips, max(1, 256 // rows))


def weights(rows):
    groups = rows // SUB
    span = LANES // groups
    k = lax.broadcasted_iota(jnp.int32, (LANES, groups * LANES), 0)
    g = lax.broadcasted_iota(jnp.int32, (LANES, groups * LANES), 1) // LANES
    weigh = jnp.zeros((LANES, groups * LANES), jnp.float32)
    for d in range(DIGITS):
        weigh = jnp.where(k == g * span + d, float(BASE**d), weigh)
    return weigh.astype(jnp.bfloat16)


class Pool:
    def __init__(self, rows, order, columns, side, pool_ref, id_ref, score_ref):
        self.rows, self.order, self.columns = rows, order, columns
        self.pool, self.id, self.score = pool_ref, id_ref, score_ref
        self.offset = side * columns * rows
        self.chips, tall, _ = pool_ref.shape
        self.cols = (tall - SUB) // rows
        self.groups = rows // SUB
        self.batch = chunk_of(self.chips, rows)
        self.blocks = self.chips // self.batch
        self.tiles = self.batch * self.groups

    def repeat(self, body, init):
        return body(0, init) if self.blocks == 1 else lax.fori_loop(0, self.blocks, body, init)

    def decode(self):
        weigh = weights(self.rows)

        def body(b, _):
            digit = self.pool[pl.ds(b * self.batch, self.batch), self.cols * self.rows :, :]
            self.id[pl.ds(b * self.batch * SUB, self.batch * SUB), :] = jnp.dot(
                digit.reshape(self.batch * SUB, LANES), weigh, preferred_element_type=jnp.float32
            )
            return 0

        self.repeat(body, 0)

    def ids(self, b, t):
        d, g = divmod(t, self.groups)
        return self.id[pl.ds((b * self.batch + d) * SUB, SUB), g * LANES : (g + 1) * LANES]

    def first(self, b, t):
        d, g = divmod(t, self.groups)
        chip = self.order[d] if self.blocks == 1 else b * self.batch + d
        return ((chip // self.columns) * 2 * self.columns + chip % self.columns) * self.rows + g * SUB

    def place(self, b, t, lane):
        return pl.ds((b * self.tiles + t) * SUB, SUB), slice(lane, lane + LANES)

    def multiply(self, users, lane):
        def body(b, _):
            size = self.batch * self.rows
            left = jnp.concatenate(
                [
                    self.pool[pl.ds(b * self.batch, self.batch), c * self.rows : (c + 1) * self.rows, :]
                    .reshape(size, LANES)
                    for c in range(self.cols)
                ],
                axis=1,
            )
            self.score[pl.ds(b * size, size), lane : lane + users.shape[0]] = lax.dot_general(
                left, users, (((1,), (1,)), ((), ())), preferred_element_type=jnp.float32
            )
            return 0

        self.repeat(body, 0)

    def find(self, wanted, lane, carry):
        where = wanted - (lax.broadcasted_iota(jnp.int32, (SUB, LANES), 0) + self.offset)

        def body(b, carry):
            own, got = carry
            for t in range(self.tiles):
                hit = where == self.first(b, t)
                own = jnp.where(hit, self.ids(b, t), own)
                got = jnp.where(hit, self.score[self.place(b, t, lane)], got)
            return own, got

        return self.repeat(body, carry)

    def mask(self, own, lane, masked_ref, to, high):
        def body(b, high):
            for t in range(self.tiles):
                masked = jnp.where(self.ids(b, t) == own, LOW, self.score[self.place(b, t, lane)])
                masked_ref[self.place(b, t, to)] = masked
                high = jnp.maximum(high, masked)
            return high

        return self.repeat(body, high)

    def add(self, masked_ref, to, high, summed):
        def body(b, summed):
            for t in range(self.tiles):
                summed = summed + jnp.exp2((masked_ref[self.place(b, t, to)] - high) * RATE)
            return summed

        return self.repeat(body, summed)


def near_kernel(rows, order, columns, wide, pool_ref, users_ref, pos_ref, score_ref, id_ref, own_ref, got_ref):
    side = (lax.axis_index("d") // columns) % 2
    pool = Pool(rows, order, columns, side, pool_ref, id_ref, score_ref)
    pool.decode()
    zero = jnp.zeros((SUB, LANES), jnp.float32)
    for u in range(0, users_ref.shape[0], wide):
        pool.multiply(users_ref[u : u + wide, :], u)
        for at in range(u, u + wide, LANES):
            own, got = pool.find(pos_ref[:, at : at + LANES], at, (zero, zero))
            own_ref[:, at : at + LANES] = own
            got_ref[:, at : at + LANES] = got


def far_kernel(
    rows, order, columns, wide, pool_ref, users_ref, pos_ref, near_ref, near_id_ref, own_ref, got_ref,
    out_ref, score_ref, id_ref, masked_ref,
):
    side = (lax.axis_index("d") // columns) % 2
    near = Pool(rows, order, columns, side, pool_ref, near_id_ref, near_ref)
    far = Pool(rows, order, columns, 1 - side, pool_ref, id_ref, score_ref)
    far.decode()
    for u in range(0, users_ref.shape[0], wide):
        far.multiply(users_ref[u : u + wide, :], 0)
        for v in range(0, wide, LANES):
            at = u + v
            carry = own_ref[:, at : at + LANES], got_ref[:, at : at + LANES]
            own, got = far.find(pos_ref[:, at : at + LANES], v, carry)
            own = jnp.broadcast_to(jnp.sum(own, axis=0, keepdims=True), (SUB, LANES))
            got = jnp.sum(got, axis=0, keepdims=True)
            high = jnp.full((SUB, LANES), LOW, jnp.float32)
            high = near.mask(own, at, masked_ref, v, high)
            high = far.mask(own, v, score_ref, v, high)
            top = jnp.maximum(jnp.max(high, axis=0, keepdims=True), got)
            high = jnp.broadcast_to(top, (SUB, LANES))
            summed = jnp.zeros((SUB, LANES), jnp.float32)
            summed = near.add(masked_ref, v, high, summed)
            summed = far.add(score_ref, v, high, summed)
            summed = jnp.sum(summed, axis=0, keepdims=True) + jnp.exp2((got - top) * RATE)
            out_ref[:, at : at + LANES] = 0.125 * (top - got) + jnp.log(summed)


def sizes(pool, count, rows):
    chips = pool.shape[0]
    return chips * rows, min(count, 2 * LANES), (chips * SUB, rows // SUB * LANES)


def start_near(pool, users, positives, rows, order, columns):
    count, width = users.shape
    tall, wide, ids = sizes(pool, count, rows)
    limit = (6 << 20) + 4 * tall * count + 4 * math.prod(ids)
    vmem = pl.BlockSpec(memory_space=pltpu.VMEM)
    return pl.pallas_call(
        functools.partial(near_kernel, rows, order, columns, wide),
        out_shape=[
            jax.ShapeDtypeStruct((tall, count), jnp.float32),
            jax.ShapeDtypeStruct(ids, jnp.float32),
            jax.ShapeDtypeStruct((SUB, count), jnp.float32),
            jax.ShapeDtypeStruct((SUB, count), jnp.float32),
        ],
        in_specs=[vmem] * 3,
        out_specs=[vmem] * 4,
        compiler_params=pltpu.CompilerParams(vmem_limit_bytes=limit + 2 * pool.nbytes),
        cost_estimate=pl.CostEstimate(
            flops=2 * tall * count * width, bytes_accessed=users.nbytes, transcendentals=0
        ),
        name="near",
    )(pool, users, positives)


def finish_far(pool, users, positives, held, rows, order, columns):
    count, width = users.shape
    tall, wide, ids = sizes(pool, count, rows)
    limit = (6 << 20) + 4 * tall * (count + 2 * wide) + 8 * math.prod(ids)
    vmem = pl.BlockSpec(memory_space=pltpu.VMEM)
    return pl.pallas_call(
        functools.partial(far_kernel, rows, order, columns, wide),
        out_shape=jax.ShapeDtypeStruct((1, count), jnp.float32),
        in_specs=[vmem] * 7,
        out_specs=vmem,
        scratch_shapes=[
            pltpu.VMEM((tall, wide), jnp.float32),
            pltpu.VMEM(ids, jnp.float32),
            pltpu.VMEM((tall, wide), jnp.float32),
        ],
        compiler_params=pltpu.CompilerParams(vmem_limit_bytes=limit + 2 * pool.nbytes),
        name="far",
    )(pool, users, positives, *held).reshape(count)


def per_device(columns, chips, users, positives, items, item_ids):
    rows = items.shape[0]
    order = list(range(chips))
    if chunk_of(chips, rows) == chips:
        random.Random(SEED).shuffle(order)

    def device(chip, side):
        return (chip // columns * 2 + side) * columns + chip % columns

    groups = [[device(chip, side) for chip in order] for side in range(2)]
    swaps = [(device(chip, side), device(chip, 1 - side)) for chip in order for side in range(2)]
    sent = pack(items, item_ids, chips)
    near = lax.all_to_all(sent, "d", 0, 0, tiled=False, axis_index_groups=groups)
    far = lax.ppermute(near, "d", swaps)
    wanted = positives.reshape(1, -1)
    held = start_near(near, users, wanted, rows, order, columns)
    return finish_far(far, users, wanted, held, rows, order, columns)


def solution(mesh):
    columns = mesh.shape["col"]
    chips = mesh.shape["row"] // 2 * columns
    flat = Mesh(mesh.devices.reshape(-1), ("d",))
    return jax.shard_map(
        functools.partial(per_device, columns, chips),
        mesh=flat,
        in_specs=(P("d", None), P("d"), P("d", None), P("d")),
        out_specs=P("d"),
        check_vma=False,
    )
```

```python
import functools
import math

import jax
import jax.numpy as jnp
from jax import lax
from jax.experimental import pallas as pl
from jax.experimental.pallas import tpu as pltpu
from jax.sharding import Mesh
from jax.sharding import PartitionSpec as P

LANES = 128
SUB = 8
BASE = 256
DIGITS = 3
LOW = -1e30
RATE = 0.125 / math.log(2)
REACH = 40.0
ORDER = (13, 4, 0, 11, 1, 5, 8, 10, 12, 2, 3, 6, 7, 14, 9, 15)
TURNED = (0, 3, 10)


def pack_kernel(items_hbm, ids_hbm, out_ref, items_ref, ids_ref, sems):
    rows, width = items_ref.shape
    groups = rows // SUB
    span = LANES // groups
    copies = out_ref.shape[0]
    get_items = pltpu.make_async_copy(items_hbm, items_ref, sems.at[0])
    get_ids = pltpu.make_async_copy(ids_hbm, ids_ref, sems.at[1])
    get_ids.start()
    get_items.start()
    row = lax.broadcasted_iota(jnp.int32, (SUB, LANES), 0)
    lane = lax.broadcasted_iota(jnp.int32, (SUB, LANES), 1)
    get_ids.wait()
    held = jnp.zeros((SUB, LANES), jnp.int32)
    for k in range(rows):
        group = k // SUB
        mine = (row == k % SUB) & (lane >= group * span) & (lane < (group + 1) * span)
        held = jnp.where(mine, ids_ref[k], held)
    place = lane % span
    digit = jnp.zeros((SUB, LANES), jnp.int32)
    for d in range(DIGITS):
        digit = jnp.where(place == d, (held // BASE**d) % BASE, digit)
    tail = digit.astype(jnp.float32).astype(jnp.bfloat16)
    get_items.wait()
    cols = [items_ref[:, c * LANES : (c + 1) * LANES] for c in range(width // LANES)]
    for n in range(copies):
        for c, col in enumerate(cols):
            out_ref[n, c * rows : (c + 1) * rows, :] = col
        out_ref[n, len(cols) * rows :, :] = tail


def pack(items, ids, copies):
    rows, width = items.shape
    tall = rows * (width // LANES) + SUB
    return pl.pallas_call(
        pack_kernel,
        out_shape=jax.ShapeDtypeStruct((copies, tall, LANES), items.dtype),
        in_specs=[pl.BlockSpec(memory_space=pltpu.HBM)] * 2,
        out_specs=pl.BlockSpec(memory_space=pltpu.VMEM),
        scratch_shapes=[
            pltpu.VMEM((rows, width), items.dtype),
            pltpu.SMEM((rows,), jnp.int32),
            pltpu.SemaphoreType.DMA((2,)),
        ],
        compiler_params=pltpu.CompilerParams(vmem_limit_bytes=(2 << 20) + 4 * copies * tall * LANES),
        cost_estimate=pl.CostEstimate(flops=1 << 30, bytes_accessed=1 << 22, transcendentals=0),
        name="pack",
    )(pltpu.with_memory_space_constraint(items, pltpu.HBM), pltpu.with_memory_space_constraint(ids, pltpu.HBM))


def chunk_of(chips, rows):
    return math.gcd(chips, max(1, 256 // rows))


def weights(rows):
    groups = rows // SUB
    span = LANES // groups
    k = lax.broadcasted_iota(jnp.int32, (LANES, groups * LANES), 0)
    g = lax.broadcasted_iota(jnp.int32, (LANES, groups * LANES), 1) // LANES
    weigh = jnp.zeros((LANES, groups * LANES), jnp.float32)
    for d in range(DIGITS):
        weigh = jnp.where(k == g * span + d, float(BASE**d), weigh)
    return weigh.astype(jnp.bfloat16)


class Pool:
    def __init__(self, rows, plan, columns, group, pool_ref, id_ref, score_ref):
        self.rows, self.columns = rows, columns
        self.order, self.turned = plan
        self.pool, self.id, self.score = pool_ref, id_ref, score_ref
        self.group = group
        self.chips, tall, _ = pool_ref.shape
        self.cols = (tall - SUB) // rows
        self.groups = rows // SUB
        self.batch = chunk_of(self.chips, rows)
        self.blocks = self.chips // self.batch
        self.tiles = self.batch * self.groups

    def repeat(self, body, init):
        return body(0, init) if self.blocks == 1 else lax.fori_loop(0, self.blocks, body, init)

    def decode(self):
        weigh = weights(self.rows)

        def body(b, _):
            digit = self.pool[pl.ds(b * self.batch, self.batch), self.cols * self.rows :, :]
            self.id[pl.ds(b * self.batch * SUB, self.batch * SUB), :] = jnp.dot(
                digit.reshape(self.batch * SUB, LANES), weigh, preferred_element_type=jnp.float32
            )
            return 0

        self.repeat(body, 0)

    def ids(self, b, t):
        d, g = divmod(t, self.groups)
        return self.id[pl.ds((b * self.batch + d) * SUB, SUB), g * LANES : (g + 1) * LANES]

    def chip(self, b, d):
        return self.order[d] if self.blocks == 1 else b * self.batch + d

    def first(self, chip, g):
        return ((chip // self.columns) * 2 * self.columns + chip % self.columns) * self.rows + g * SUB

    def place(self, b, t, lane):
        return pl.ds((b * self.tiles + t) * SUB, SUB), pl.ds(lane, LANES)

    def multiply(self, users, lane):
        def body(b, _):
            size = self.batch * self.rows
            left = jnp.concatenate(
                [
                    self.pool[pl.ds(b * self.batch, self.batch), c * self.rows : (c + 1) * self.rows, :]
                    .reshape(size, LANES)
                    for c in range(self.cols)
                ],
                axis=1,
            )
            self.score[pl.ds(b * size, size), lane : lane + users.shape[0]] = lax.dot_general(
                left, users, (((1,), (1,)), ((), ())), preferred_element_type=jnp.float32
            )
            return 0

        self.repeat(body, 0)

    def find(self, wanted, lane, carry):
        up = lax.broadcasted_iota(jnp.int32, (SUB, LANES), 0)
        step = self.columns * self.rows
        straight = wanted - (up + self.group * step)
        crossed = wanted - (up + (1 - self.group) * step) if self.turned else straight

        def body(b, carry):
            own, got, peak = carry
            for t in range(self.tiles):
                chip = self.chip(b, t // self.groups)
                where = crossed if self.turned and chip in self.turned else straight
                hit = where == self.first(chip, t % self.groups)
                score = self.score[self.place(b, t, lane)]
                own = jnp.where(hit, self.ids(b, t), own)
                got = jnp.where(hit, score, got)
                peak = jnp.maximum(peak, score)
            return own, got, peak

        return self.repeat(body, carry)

    def raise_to(self, lane, high, term_ref):
        def body(b, _):
            for t in range(self.tiles):
                at = self.place(b, t, lane)
                term_ref[at] = jnp.exp2((self.score[at] - high) * RATE)
            return 0

        self.repeat(body, 0)

    def add_raised(self, own, lane, term_ref, summed):
        def body(b, summed):
            for t in range(self.tiles):
                summed = summed + jnp.where(self.ids(b, t) == own, 0.0, term_ref[self.place(b, t, lane)])
            return summed

        return self.repeat(body, summed)

    def kept(self, own, b, t, lane):
        return jnp.where(self.ids(b, t) == own, LOW, self.score[self.place(b, t, lane)])

    def add(self, own, lane, high, summed):
        def body(b, summed):
            for t in range(self.tiles):
                summed = summed + jnp.exp2((self.kept(own, b, t, lane) - high) * RATE)
            return summed

        return self.repeat(body, summed)

    def highest(self, own, lane, high):
        def body(b, high):
            for t in range(self.tiles):
                high = jnp.maximum(high, self.kept(own, b, t, lane))
            return high

        return self.repeat(body, high)


def spread(row):
    return jnp.broadcast_to(row, (SUB, LANES))


def total(x):
    return jnp.sum(x, axis=0, keepdims=True)


def group_of(columns, turned):
    row, column = lax.axis_index("d") // columns, lax.axis_index("d") % columns
    chip = row // 2 * columns + column
    flips = sum(1 << k for k in turned)
    return row % 2 if not turned else (row + (lax.shift_right_logical(jnp.int32(flips), chip) & 1)) % 2


def near_kernel(
    rows, plan, columns, wide, pool_ref, users_ref, pos_ref,
    score_ref, id_ref, own_ref, got_ref, top_ref, *term_ref,
):
    group = group_of(columns, plan[1])
    pool = Pool(rows, plan, columns, group, pool_ref, id_ref, score_ref)
    pool.decode()
    zero = jnp.zeros((SUB, LANES), jnp.float32)
    for u in range(0, users_ref.shape[0], wide):
        pool.multiply(users_ref[u : u + wide, :], u)
        for at in range(u, u + wide, LANES):
            here = pl.ds(at, LANES)
            own, got, peak = pool.find(pos_ref[:, here], at, (zero, zero, zero + LOW))
            own_ref[:, here] = own
            got_ref[:, here] = got
            top = jnp.max(peak, axis=0, keepdims=True)
            top_ref[:, here] = top
            if term_ref:
                pool.raise_to(at, spread(top), term_ref[0])


def far_kernel(
    rows, plan, columns, wide, pool_ref, users_ref, pos_ref, near_ref, near_id_ref, own_ref, got_ref, top_ref,
    *refs,
):
    term_ref = refs[:-5]
    out_hbm, out_ref, score_ref, id_ref, sem = refs[-5:]
    group = group_of(columns, plan[1])
    near = Pool(rows, plan, columns, group, pool_ref, near_id_ref, near_ref)
    far = Pool(rows, plan, columns, 1 - group, pool_ref, id_ref, score_ref)
    zero = jnp.zeros((SUB, LANES), jnp.float32)

    def settle(lane, got, top, summed):
        summed = total(summed) + jnp.exp2((got - top) * RATE)
        out_ref[:, pl.ds(lane, LANES)] = 0.125 * (top - got) + jnp.log(summed)

    def find(lane, base):
        here = pl.ds(lane, LANES)
        carry = own_ref[:, here], got_ref[:, here], zero + LOW
        own, got, peak = far.find(pos_ref[:, here], base, carry)
        return spread(total(own)), total(got), jnp.max(peak, axis=0, keepdims=True)

    def careful(lane, base, own, got):
        high = far.highest(own, base, near.highest(own, lane, zero + LOW))
        top = jnp.maximum(jnp.max(high, axis=0, keepdims=True), got)
        summed = near.add(own, lane, spread(top), zero)
        summed = far.add(own, base, spread(top), summed)
        settle(lane, got, top, summed)

    far.decode()
    worst = jnp.zeros((1, LANES), jnp.float32)
    for u in range(0, users_ref.shape[0], wide):
        start = u if term_ref else 0
        far.multiply(users_ref[u : u + wide, :], start)
        for v in range(0, wide, LANES):
            lane, base = u + v, start + v
            own, got, peak = find(lane, base)
            if not term_ref:
                careful(lane, base, own, got)
                continue
            near_top = top_ref[:, pl.ds(lane, LANES)]
            top = jnp.maximum(peak, near_top)
            worst = jnp.maximum(worst, top - got)
            summed = near.add_raised(own, lane, term_ref[0], zero)
            summed = summed * spread(jnp.exp2((near_top - top) * RATE))
            summed = far.add(own, base, spread(top), summed)
            settle(lane, got, top, summed)

    copy = pltpu.make_async_copy(out_ref, out_hbm, sem)
    copy.start()
    if term_ref:

        @pl.when(jnp.max(worst) * RATE > REACH)
        def _():
            copy.wait()

            @pl.loop(0, out_ref.shape[1] // LANES)
            def _(n):
                lane = pl.multiple_of(n * LANES, LANES)
                own, got, _ = find(lane, lane)
                careful(lane, lane, own, got)

            copy.start()

    copy.wait()


def one_block(pool, rows):
    return chunk_of(pool.shape[0], rows) == pool.shape[0]


def sizes(pool, count, rows):
    chips = pool.shape[0]
    return chips * rows, min(count, 2 * LANES), (chips * SUB, rows // SUB * LANES)


def start_near(pool, users, positives, rows, plan, columns):
    count, width = users.shape
    tall, wide, ids = sizes(pool, count, rows)
    raised = [jax.ShapeDtypeStruct((tall, count), jnp.float32)] if one_block(pool, rows) else []
    limit = (6 << 20) + 4 * tall * count * (1 + len(raised)) + 4 * math.prod(ids)
    vmem = pl.BlockSpec(memory_space=pltpu.VMEM)
    return pl.pallas_call(
        functools.partial(near_kernel, rows, plan, columns, wide),
        out_shape=[
            jax.ShapeDtypeStruct((tall, count), jnp.float32),
            jax.ShapeDtypeStruct(ids, jnp.float32),
            jax.ShapeDtypeStruct((SUB, count), jnp.float32),
            jax.ShapeDtypeStruct((SUB, count), jnp.float32),
            jax.ShapeDtypeStruct((1, count), jnp.float32),
            *raised,
        ],
        in_specs=[vmem] * 3,
        out_specs=[vmem] * (5 + len(raised)),
        compiler_params=pltpu.CompilerParams(vmem_limit_bytes=limit + 2 * pool.nbytes),
        cost_estimate=pl.CostEstimate(
            flops=2 * tall * count * width, bytes_accessed=users.nbytes, transcendentals=0
        ),
        name="near",
    )(pool, users, positives)


def finish_far(pool, users, positives, held, rows, plan, columns):
    count, width = users.shape
    tall, wide, ids = sizes(pool, count, rows)
    across = count if one_block(pool, rows) else wide
    limit = (6 << 20) + 4 * tall * ((len(held) - 4) * count + across) + 8 * math.prod(ids)
    vmem = pl.BlockSpec(memory_space=pltpu.VMEM)
    return pl.pallas_call(
        functools.partial(far_kernel, rows, plan, columns, wide),
        out_shape=jax.ShapeDtypeStruct((1, count), jnp.float32),
        in_specs=[vmem] * (3 + len(held)),
        out_specs=pl.BlockSpec(memory_space=pltpu.HBM),
        scratch_shapes=[
            pltpu.VMEM((1, count), jnp.float32),
            pltpu.VMEM((tall, across), jnp.float32),
            pltpu.VMEM(ids, jnp.float32),
            pltpu.SemaphoreType.DMA,
        ],
        compiler_params=pltpu.CompilerParams(vmem_limit_bytes=limit + 2 * pool.nbytes),
        name="far",
    )(pool, users, positives, *held).reshape(count)


def per_device(columns, chips, users, positives, items, item_ids):
    rows = items.shape[0]
    order, turned = list(range(chips)), ()
    if chunk_of(chips, rows) == chips:
        size = len(ORDER)
        order.sort(key=lambda chip: (ORDER.index(chip % size), chip))
        turned = tuple(chip for chip in order if chip % size in TURNED)
    plan = tuple(order), turned

    def device(chip, side):
        return (chip // columns * 2 + (side ^ (chip in turned))) * columns + chip % columns

    groups = [[device(chip, side) for chip in order] for side in range(2)]
    swaps = [(device(chip, side), device(chip, 1 - side)) for chip in order for side in range(2)]
    sent = pack(items, item_ids, chips)
    near = lax.all_to_all(sent, "d", 0, 0, tiled=False, axis_index_groups=groups)
    far = lax.ppermute(near, "d", swaps)
    wanted = positives.reshape(1, -1)
    held = start_near(near, users, wanted, rows, plan, columns)
    return finish_far(far, users, wanted, held, rows, plan, columns)


def solution(mesh):
    columns = mesh.shape["col"]
    chips = mesh.shape["row"] // 2 * columns
    flat = Mesh(mesh.devices.reshape(-1), ("d",))
    return jax.shard_map(
        functools.partial(per_device, columns, chips),
        mesh=flat,
        in_specs=(P("d", None), P("d"), P("d", None), P("d")),
        out_specs=P("d"),
        check_vma=False,
    )
```

```python
import functools
import math

import jax
import jax.numpy as jnp
from jax import lax
from jax.experimental import pallas as pl
from jax.experimental.pallas import tpu as pltpu
from jax.sharding import Mesh
from jax.sharding import PartitionSpec as P

LANES = 128
SUB = 8
BASE = 256
DIGITS = 3
LOW = -1e30
RATE = 0.125 / math.log(2)
REACH = 40.0
ORDER = (13, 4, 0, 11, 1, 5, 8, 10, 12, 2, 3, 6, 7, 14, 9, 15)
TURNED = (0, 3, 10)


def pack_kernel(items_hbm, ids_hbm, out_ref, items_ref, ids_ref, sems):
    rows, width = items_ref.shape
    groups = rows // SUB
    span = LANES // groups
    copies = out_ref.shape[0]
    get_items = pltpu.make_async_copy(items_hbm, items_ref, sems.at[0])
    get_ids = pltpu.make_async_copy(ids_hbm, ids_ref, sems.at[1])
    get_ids.start()
    get_items.start()
    row = lax.broadcasted_iota(jnp.int32, (SUB, LANES), 0)
    lane = lax.broadcasted_iota(jnp.int32, (SUB, LANES), 1)
    get_ids.wait()
    held = jnp.zeros((SUB, LANES), jnp.int32)
    for k in range(rows):
        group = k // SUB
        mine = (row == k % SUB) & (lane >= group * span) & (lane < (group + 1) * span)
        held = jnp.where(mine, ids_ref[k], held)
    place = lane % span
    digit = jnp.zeros((SUB, LANES), jnp.int32)
    for d in range(DIGITS):
        digit = jnp.where(place == d, (held // BASE**d) % BASE, digit)
    tail = digit.astype(jnp.float32).astype(jnp.bfloat16)
    get_items.wait()
    cols = [items_ref[:, c * LANES : (c + 1) * LANES] for c in range(width // LANES)]
    for n in range(copies):
        for c, col in enumerate(cols):
            out_ref[n, c * rows : (c + 1) * rows, :] = col
        out_ref[n, len(cols) * rows :, :] = tail


def pack(items, ids, copies):
    rows, width = items.shape
    tall = rows * (width // LANES) + SUB
    return pl.pallas_call(
        pack_kernel,
        out_shape=jax.ShapeDtypeStruct((copies, tall, LANES), items.dtype),
        in_specs=[pl.BlockSpec(memory_space=pltpu.HBM)] * 2,
        out_specs=pl.BlockSpec(memory_space=pltpu.VMEM),
        scratch_shapes=[
            pltpu.VMEM((rows, width), items.dtype),
            pltpu.SMEM((rows,), jnp.int32),
            pltpu.SemaphoreType.DMA((2,)),
        ],
        compiler_params=pltpu.CompilerParams(vmem_limit_bytes=(2 << 20) + 4 * copies * tall * LANES),
        cost_estimate=pl.CostEstimate(flops=1 << 30, bytes_accessed=1 << 22, transcendentals=0),
        name="pack",
    )(pltpu.with_memory_space_constraint(items, pltpu.HBM), pltpu.with_memory_space_constraint(ids, pltpu.HBM))


def chunk_of(chips, rows):
    return math.gcd(chips, max(1, 256 // rows))


def weights(rows):
    groups = rows // SUB
    span = LANES // groups
    k = lax.broadcasted_iota(jnp.int32, (LANES, groups * LANES), 0)
    g = lax.broadcasted_iota(jnp.int32, (LANES, groups * LANES), 1) // LANES
    weigh = jnp.zeros((LANES, groups * LANES), jnp.float32)
    for d in range(DIGITS):
        weigh = jnp.where(k == g * span + d, float(BASE**d), weigh)
    return weigh.astype(jnp.bfloat16)


class Pool:
    def __init__(self, rows, plan, columns, group, pool_ref, id_ref, score_ref):
        self.rows, self.columns = rows, columns
        self.order, self.turned = plan
        self.pool, self.id, self.score = pool_ref, id_ref, score_ref
        self.group = group
        self.chips, tall, _ = pool_ref.shape
        self.cols = (tall - SUB) // rows
        self.groups = rows // SUB
        self.batch = chunk_of(self.chips, rows)
        self.blocks = self.chips // self.batch
        self.tiles = self.batch * self.groups

    def repeat(self, body, init):
        return body(0, init) if self.blocks == 1 else lax.fori_loop(0, self.blocks, body, init)

    def decode(self, weigh):
        def body(b, _):
            digit = self.pool[pl.ds(b * self.batch, self.batch), self.cols * self.rows :, :]
            self.id[pl.ds(b * self.batch * SUB, self.batch * SUB), :] = jnp.dot(
                digit.reshape(self.batch * SUB, LANES), weigh, preferred_element_type=jnp.float32
            )
            return 0

        self.repeat(body, 0)

    def ids(self, b, t):
        d, g = divmod(t, self.groups)
        return self.id[pl.ds((b * self.batch + d) * SUB, SUB), g * LANES : (g + 1) * LANES]

    def chip(self, b, d):
        return self.order[d] if self.blocks == 1 else b * self.batch + d

    def first(self, chip, g):
        return ((chip // self.columns) * 2 * self.columns + chip % self.columns) * self.rows + g * SUB

    def place(self, b, t, lane):
        return pl.ds((b * self.tiles + t) * SUB, SUB), pl.ds(lane, LANES)

    def multiply(self, users, lane):
        def body(b, _):
            size = self.batch * self.rows
            left = jnp.concatenate(
                [
                    self.pool[pl.ds(b * self.batch, self.batch), c * self.rows : (c + 1) * self.rows, :]
                    .reshape(size, LANES)
                    for c in range(self.cols)
                ],
                axis=1,
            )
            self.score[pl.ds(b * size, size), lane : lane + users.shape[0]] = lax.dot_general(
                left, users, (((1,), (1,)), ((), ())), preferred_element_type=jnp.float32
            )
            return 0

        self.repeat(body, 0)

    def find(self, wanted, lane, carry):
        up = lax.broadcasted_iota(jnp.int32, (SUB, LANES), 0)
        step = self.columns * self.rows
        straight = wanted - (up + self.group * step)
        crossed = wanted - (up + (1 - self.group) * step) if self.turned else straight

        def body(b, carry):
            own, got, peak = carry
            for t in range(self.tiles):
                chip = self.chip(b, t // self.groups)
                where = crossed if self.turned and chip in self.turned else straight
                hit = where == self.first(chip, t % self.groups)
                score = self.score[self.place(b, t, lane)]
                own = jnp.where(hit, self.ids(b, t), own)
                got = jnp.where(hit, score, got)
                peak = jnp.maximum(peak, score)
            return own, got, peak

        return self.repeat(body, carry)

    def raise_to(self, lane, high, term_ref):
        def body(b, _):
            for t in range(self.tiles):
                at = self.place(b, t, lane)
                term_ref[at] = jnp.exp2((self.score[at] - high) * RATE)
            return 0

        self.repeat(body, 0)

    def add_raised(self, own, lane, term_ref, summed):
        def body(b, summed):
            for t in range(self.tiles):
                summed = summed + jnp.where(self.ids(b, t) == own, 0.0, term_ref[self.place(b, t, lane)])
            return summed

        return self.repeat(body, summed)

    def kept(self, own, b, t, lane):
        return jnp.where(self.ids(b, t) == own, LOW, self.score[self.place(b, t, lane)])

    def add(self, own, lane, high, summed):
        def body(b, summed):
            for t in range(self.tiles):
                summed = summed + jnp.exp2((self.kept(own, b, t, lane) - high) * RATE)
            return summed

        return self.repeat(body, summed)

    def highest(self, own, lane, high):
        def body(b, high):
            for t in range(self.tiles):
                high = jnp.maximum(high, self.kept(own, b, t, lane))
            return high

        return self.repeat(body, high)


def spread(row):
    return jnp.broadcast_to(row, (SUB, LANES))


def total(x):
    return jnp.sum(x, axis=0, keepdims=True)


def group_of(columns, turned):
    row, column = lax.axis_index("d") // columns, lax.axis_index("d") % columns
    chip = row // 2 * columns + column
    flips = sum(1 << k for k in turned)
    return row % 2 if not turned else (row + (lax.shift_right_logical(jnp.int32(flips), chip) & 1)) % 2


def near_kernel(
    rows, plan, columns, wide, pool_ref, users_ref, pos_ref,
    score_ref, id_ref, own_ref, got_ref, top_ref, weigh_ref, *term_ref,
):
    group = group_of(columns, plan[1])
    pool = Pool(rows, plan, columns, group, pool_ref, id_ref, score_ref)
    weigh = weights(rows)
    weigh_ref[...] = weigh
    pool.decode(weigh)
    zero = jnp.zeros((SUB, LANES), jnp.float32)
    for u in range(0, users_ref.shape[0], wide):
        pool.multiply(users_ref[u : u + wide, :], u)
        for at in range(u, u + wide, LANES):
            here = pl.ds(at, LANES)
            own, got, peak = pool.find(pos_ref[:, here], at, (zero, zero, zero + LOW))
            own_ref[:, here] = own
            got_ref[:, here] = got
            top = jnp.max(peak, axis=0, keepdims=True)
            top_ref[:, here] = top
            if term_ref:
                pool.raise_to(at, spread(top), term_ref[0])


def far_kernel(
    rows, plan, columns, wide, pool_ref, users_ref, pos_ref, near_ref, near_id_ref, own_ref, got_ref, top_ref,
    weigh_ref, *refs,
):
    term_ref = refs[:-5]
    out_hbm, out_ref, score_ref, id_ref, sem = refs[-5:]
    group = group_of(columns, plan[1])
    near = Pool(rows, plan, columns, group, pool_ref, near_id_ref, near_ref)
    far = Pool(rows, plan, columns, 1 - group, pool_ref, id_ref, score_ref)
    zero = jnp.zeros((SUB, LANES), jnp.float32)

    def settle(lane, got, top, summed):
        summed = total(summed) + jnp.exp2((got - top) * RATE)
        out_ref[:, pl.ds(lane, LANES)] = 0.125 * (top - got) + jnp.log(summed)

    def find(lane, base):
        here = pl.ds(lane, LANES)
        carry = own_ref[:, here], got_ref[:, here], zero + LOW
        own, got, peak = far.find(pos_ref[:, here], base, carry)
        return spread(total(own)), total(got), jnp.max(peak, axis=0, keepdims=True)

    def careful(lane, base, own, got):
        high = far.highest(own, base, near.highest(own, lane, zero + LOW))
        top = jnp.maximum(jnp.max(high, axis=0, keepdims=True), got)
        summed = near.add(own, lane, spread(top), zero)
        summed = far.add(own, base, spread(top), summed)
        settle(lane, got, top, summed)

    far.decode(weigh_ref[...])
    worst = jnp.zeros((1, LANES), jnp.float32)
    for u in range(0, users_ref.shape[0], wide):
        start = u if term_ref else 0
        far.multiply(users_ref[u : u + wide, :], start)
        for v in range(0, wide, LANES):
            lane, base = u + v, start + v
            own, got, peak = find(lane, base)
            if not term_ref:
                careful(lane, base, own, got)
                continue
            near_top = top_ref[:, pl.ds(lane, LANES)]
            top = jnp.maximum(peak, near_top)
            worst = jnp.maximum(worst, top - got)
            summed = near.add_raised(own, lane, term_ref[0], zero)
            summed = summed * spread(jnp.exp2((near_top - top) * RATE))
            summed = far.add(own, base, spread(top), summed)
            settle(lane, got, top, summed)

    copy = pltpu.make_async_copy(out_ref, out_hbm, sem)
    copy.start()
    if term_ref:

        @pl.when(jnp.max(worst) * RATE > REACH)
        def _():
            copy.wait()

            @pl.loop(0, out_ref.shape[1] // LANES)
            def _(n):
                lane = pl.multiple_of(n * LANES, LANES)
                own, got, _ = find(lane, lane)
                careful(lane, lane, own, got)

            copy.start()

    copy.wait()


def one_block(pool, rows):
    return chunk_of(pool.shape[0], rows) == pool.shape[0]


def sizes(pool, count, rows):
    chips = pool.shape[0]
    return chips * rows, min(count, 2 * LANES), (chips * SUB, rows // SUB * LANES)


def start_near(pool, users, positives, rows, plan, columns):
    count, width = users.shape
    tall, wide, ids = sizes(pool, count, rows)
    raised = [jax.ShapeDtypeStruct((tall, count), jnp.float32)] if one_block(pool, rows) else []
    limit = (6 << 20) + 4 * tall * count * (1 + len(raised)) + 4 * math.prod(ids)
    vmem = pl.BlockSpec(memory_space=pltpu.VMEM)
    return pl.pallas_call(
        functools.partial(near_kernel, rows, plan, columns, wide),
        out_shape=[
            jax.ShapeDtypeStruct((tall, count), jnp.float32),
            jax.ShapeDtypeStruct(ids, jnp.float32),
            jax.ShapeDtypeStruct((SUB, count), jnp.float32),
            jax.ShapeDtypeStruct((SUB, count), jnp.float32),
            jax.ShapeDtypeStruct((1, count), jnp.float32),
            jax.ShapeDtypeStruct((LANES, rows // SUB * LANES), jnp.bfloat16),
            *raised,
        ],
        in_specs=[vmem] * 3,
        out_specs=[vmem] * (6 + len(raised)),
        compiler_params=pltpu.CompilerParams(vmem_limit_bytes=limit + 2 * pool.nbytes),
        cost_estimate=pl.CostEstimate(
            flops=2 * tall * count * width, bytes_accessed=users.nbytes, transcendentals=0
        ),
        name="near",
    )(pool, users, positives)


def finish_far(pool, users, positives, held, rows, plan, columns):
    count, width = users.shape
    tall, wide, ids = sizes(pool, count, rows)
    across = count if one_block(pool, rows) else wide
    limit = (6 << 20) + 4 * tall * ((len(held) - 5) * count + across) + 8 * math.prod(ids)
    vmem = pl.BlockSpec(memory_space=pltpu.VMEM)
    return pl.pallas_call(
        functools.partial(far_kernel, rows, plan, columns, wide),
        out_shape=jax.ShapeDtypeStruct((1, count), jnp.float32),
        in_specs=[vmem] * (3 + len(held)),
        out_specs=pl.BlockSpec(memory_space=pltpu.HBM),
        scratch_shapes=[
            pltpu.VMEM((1, count), jnp.float32),
            pltpu.VMEM((tall, across), jnp.float32),
            pltpu.VMEM(ids, jnp.float32),
            pltpu.SemaphoreType.DMA,
        ],
        compiler_params=pltpu.CompilerParams(
            vmem_limit_bytes=limit + 2 * pool.nbytes
        ),
        name="far",
    )(pool, users, positives, *held).reshape(count)


def per_device(columns, chips, users, positives, items, item_ids):
    rows = items.shape[0]
    order, turned = list(range(chips)), ()
    if chunk_of(chips, rows) == chips:
        size = len(ORDER)
        order.sort(key=lambda chip: (ORDER.index(chip % size), chip))
        turned = tuple(chip for chip in order if chip % size in TURNED)
    plan = tuple(order), turned

    def device(chip, side):
        return (chip // columns * 2 + (side ^ (chip in turned))) * columns + chip % columns

    groups = [[device(chip, side) for chip in order] for side in range(2)]
    swaps = [(device(chip, side), device(chip, 1 - side)) for chip in order for side in range(2)]
    sent = pack(items, item_ids, chips)
    near = lax.all_to_all(sent, "d", 0, 0, tiled=False, axis_index_groups=groups)
    far = lax.ppermute(near, "d", swaps)
    wanted = positives.reshape(1, -1)
    held = start_near(near, users, wanted, rows, plan, columns)
    return finish_far(far, users, wanted, held, rows, plan, columns)


def solution(mesh):
    columns = mesh.shape["col"]
    chips = mesh.shape["row"] // 2 * columns
    flat = Mesh(mesh.devices.reshape(-1), ("d",))
    return jax.shard_map(
        functools.partial(per_device, columns, chips),
        mesh=flat,
        in_specs=(P("d", None), P("d"), P("d", None), P("d")),
        out_specs=P("d"),
        check_vma=False,
    )
```
